32 devices in a mesh: src: 4 (over y, core), tgt: 8 (over z, x).
Axes of the slice: x: 2, y: 2, z: 4, core: 2. Of those that a mesh axis runs over, the one named last changes fastest.
Arguments:
- sources: float32 [256, 8192], P('tgt', 'src'), may hold values from -24 to 24, as said below
- targets: float32 [256, 8192], P('src', 'tgt'), may hold values from -24 to 24, as said below
- source_logw: float32 [8192], P('src'), may hold values from -1 to 1
- target_logw: float32 [8192], P('tgt'), may hold values from -1 to 1
- times: float32 [8192], P('src'), may hold values from 0 to 1
Outputs:
- row_potential: float32 [8192], P('src')
- moved: float32 [256, 8192], P('tgt', 'src')
- col_potential: float32 [8192], P('tgt')
The draws below stay inside these ranges and needn't reach their ends.
Inputs may be any that keep to these rules, and one draw needn't show every extreme that they name: `sources`: point coordinates. `targets`: point coordinates.
All inputs are finite; a program needn't handle non-finite values.
Results may differ from the reference program's by a relative error of at most 0.00025.
Values sent between devices are 32-bit elements; how exact they have to be, the bound alone decides.
No kernel may reach another device: no remote copies, remote signals or barrier semaphores. Data moves between devices by JAX's collectives and lax.ppermute only.
A program may use at most 64 MiB of HBM per device.

```python
import math
import jax
import jax.numpy as jnp
import numpy as np
from jax import lax

F = 256
ITERS = 2
NS = 8192
NT = 8192


def paired_points(key):
    keys = jax.random.split(jax.random.fold_in(key, 7), 5)
    clusters = max(NT // 32, 4)
    spread = math.sqrt(32.0 / math.sqrt(2.0 * F))
    centre_scale = math.sqrt(240.0 / F)
    centres = centre_scale * jax.random.normal(keys[0], (clusters, F), jnp.float32)
    target_ids = jax.random.randint(keys[1], (NT,), 0, clusters)
    source_ids = jax.random.randint(keys[2], (NS,), 0, clusters)
    target_pts = centres[target_ids] + spread * jax.random.normal(keys[3], (NT, F), jnp.float32)
    source_pts = centres[source_ids] + spread * jax.random.normal(keys[4], (NS, F), jnp.float32)
    far_rows = np.arange(4) * (NS // 4) + 2
    offset = 68.0 / math.sqrt(F)
    source_pts = source_pts.at[far_rows].add(offset)
    return (jnp.clip(source_pts, -24.0, 24.0), jnp.clip(target_pts, -24.0, 24.0))


def draw_sources(key, part):
    return paired_points(key)[0].T


def draw_targets(key, part):
    return paired_points(key)[1].T


def steps_of(key, extent, pieces, smallest, top_value):
    def one(position, blocks):
        heights = jax.random.uniform(jax.random.fold_in(jax.random.fold_in(key, 6), position), (blocks,), jnp.float32, smallest / len(pieces), top_value / len(pieces))
        return jnp.repeat(jnp.exp(heights), extent[position] // blocks).reshape((-1,) + (1,) * (len(extent) - position - 1))

    level = one(*pieces[0])
    for cut in pieces[1:]:
        level = level * one(*cut)
    return level


def setup_inputs(seed: int = 0) -> dict:
    key_list = jax.random.split(jax.random.key(seed), 6)
    sources = draw_sources(jax.random.fold_in(key_list[5], 71), 0)
    targets = draw_targets(jax.random.fold_in(key_list[5], 71), 0)
    source_logw = jnp.clip(jax.random.uniform(key_list[2], (NS,), jnp.float32, -1.0, 1.0) * steps_of(key_list[2], (NS,), ((0, 4),), -0.4, 0.0), -1.0, 1.0)
    target_logw = jnp.clip(jax.random.uniform(key_list[3], (NT,), jnp.float32, -1.0, 1.0) * steps_of(key_list[3], (NT,), ((0, 8),), -0.4, 0.0), -1.0, 1.0)
    times = jnp.clip(1.0 * jax.random.uniform(key_list[4], (NS,), jnp.float32) ** steps_of(key_list[4], (NS,), ((0, 4),), -0.2, 0.2), 0.0, 1.0)
    return {"sources": sources, "targets": targets, "source_logw": source_logw, "target_logw": target_logw, "times": times}


EPSILON = 16.0


def cost_block(rows, cols):
    cross = jnp.dot(rows, cols.T, precision=lax.Precision.HIGHEST, preferred_element_type=jnp.float32)
    return 0.5 * jnp.sum(rows * rows, 1)[:, None] + 0.5 * jnp.sum(cols * cols, 1)[None, :] - cross


def row_lse(points, targets, col_pot, block):
    count = points.shape[0] // block

    def one(blk):
        scores = (col_pot[None, :] - cost_block(blk, targets)) / EPSILON
        top = jnp.max(scores, 1)
        return top + jnp.log(jnp.sum(jnp.exp(scores - top[:, None]), 1))

    return lax.map(one, points.reshape(count, block, points.shape[1])).reshape(points.shape[0])


def col_lse(points, targets, row_pot, block):
    count = points.shape[0] // block
    cols = targets.shape[0]

    def step(carry, item):
        top, total = carry
        blk, pot = item
        scores = (pot[:, None] - cost_block(blk, targets)) / EPSILON
        fresh = jnp.maximum(top, jnp.max(scores, 0))
        total = total * jnp.exp(top - fresh) + jnp.sum(jnp.exp(scores - fresh[None, :]), 0)
        return (fresh, total), None

    init = (jnp.full((cols,), -1e30, jnp.float32), jnp.zeros((cols,), jnp.float32))
    (top, total), _ = lax.scan(step, init, (points.reshape(count, block, points.shape[1]), row_pot.reshape(count, block)))
    return top + jnp.log(total)


def reference(sources, targets, source_logw, target_logw, times):
    sources = sources.T
    targets = targets.T
    block = min(512, NS)
    col_pot = jnp.zeros((NT,), jnp.float32)
    row_pot = jnp.zeros((NS,), jnp.float32)
    for sweep in range(ITERS):
        row_pot = EPSILON * (source_logw - row_lse(sources, targets, col_pot, block))
        col_pot = EPSILON * (target_logw - col_lse(sources, targets, row_pot, block))
    count = NS // block

    def transport(item):
        blk, pot = item
        plan = jnp.exp((pot[:, None] + col_pot[None, :] - cost_block(blk, targets)) / EPSILON)
        weighted = jnp.dot(plan, targets, precision=lax.Precision.HIGHEST, preferred_element_type=jnp.float32)
        return weighted, jnp.sum(plan, 1)

    weighted, mass = lax.map(transport, (sources.reshape(count, block, F), row_pot.reshape(count, block)))
    weighted = weighted.reshape(NS, F)
    mass = mass.reshape(NS)
    moved = (1.0 - times)[:, None] * sources + times[:, None] * (weighted / mass[:, None])
    final_pot = EPSILON * (target_logw - col_lse(moved, targets, row_pot, block))
    return row_pot, moved.T, final_pot
```

```python
import jax
import jax.numpy as jnp
from jax import lax
from jax.experimental import pallas as pl
from jax.experimental.pallas import tpu as pltpu
from jax.sharding import PartitionSpec as P

EPS = 16.0
LOG2E = 1.4426950408889634
LN2 = 0.6931471805599453
L = LOG2E / EPS
LANES = 128
F32 = jnp.float32
BF16 = jnp.bfloat16
MB = 1024 * 1024


def split(v):
    hi = v.astype(BF16)
    return hi, (v - hi.astype(F32)).astype(BF16)


def dot3(ah, al, bh, bl, dims):
    d = lambda p, q: lax.dot_general(p, q, (dims, ((), ())), preferred_element_type=F32)
    return d(ah, bh) + d(ah, bl) + d(al, bh)


def to_col(row):
    return jnp.broadcast_to(row, (LANES, LANES)).T


def log2(v):
    return jnp.log(v) * LOG2E


def groups(v):
    return v.reshape(v.shape[0] // 8, 8, v.shape[1])


def call(body, outs, scratch, limit):
    return pl.pallas_call(
        body,
        out_shape=outs,
        scratch_shapes=scratch,
        compiler_params=pltpu.CompilerParams(vmem_limit_bytes=limit * MB),
    )


def kernels(F, M, N, fs, ft, A, Y, half, pb):
    nl = N // LANES
    nr = M // LANES
    sds = jax.ShapeDtypeStruct

    def cross_body(place, own, other, *refs):
        pieces = refs[: A * Y]
        s_ref, xt_ref, yh_ref, yl_ref, hy_ref, rowc_ref, logb_ref, stat_ref = refs[A * Y : A * Y + 8]
        x_ref, y_ref, xh_ref, xl_ref = refs[A * Y + 8 :]
        y, c, a, b = place[0], place[1], place[2], place[3]
        for k in range(A):
            for q in range(2):
                at = pl.multiple_of(((a ^ k) * 2 + (b ^ q)) * ft, 8)
                src = pl.ds((q * A + k) * ft, ft)
                x_ref[pl.ds(at, ft), pl.ds(pl.multiple_of(c * pb, LANES), pb)] = own[src, :]
                x_ref[pl.ds(at, ft), pl.ds(pl.multiple_of((1 - c) * pb, LANES), pb)] = other[src, :]
        rowc_ref[0:2, pl.ds(pl.multiple_of(c * pb, LANES), pb)] = own[F : F + 2, :]
        rowc_ref[0:2, pl.ds(pl.multiple_of((1 - c) * pb, LANES), pb)] = other[F : F + 2, :]
        for k in range(A):
            cols = pl.ds(pl.multiple_of((a ^ k) * half, LANES), half)
            for m in range(Y):
                p = pieces[k * Y + m]
                for q in range(2):
                    at = pl.multiple_of(((y ^ m) * 2 + (c ^ q)) * fs, 8)
                    y_ref[pl.ds(at, fs), cols] = p[q * fs : (q + 1) * fs, :]
            logb_ref[0:1, cols] = pieces[k * Y][2 * fs : 2 * fs + 1, :]
        for j in range(N // 256):
            cols = slice(j * 256, (j + 1) * 256)
            v = y_ref[:, cols]
            hy_ref[0:1, cols] = (0.5 * L) * jnp.sum(v * v, 0, keepdims=True)
            yh_ref[:, cols], yl_ref[:, cols] = split(v)
        for r in range(nr):
            rows = slice(r * LANES, (r + 1) * LANES)
            v = x_ref[:, rows]
            rowc_ref[2:3, rows] = (0.5 * L) * jnp.sum(v * v, 0, keepdims=True)
            vt = v.T
            xt_ref[rows, :] = vt
            xh_ref[rows, :], xl_ref[rows, :] = split(vt * L)
        wide = 512
        deep = min(256, M)
        for r in range(M // deep):
            rows = slice(r * deep, (r + 1) * deep)
            for j in range(N // wide):
                cols = slice(j * wide, (j + 1) * wide)
                s = dot3(xh_ref[rows, :], xl_ref[rows, :], yh_ref[:, cols], yl_ref[:, cols], ((1,), (0,)))
                s_ref[rows, cols] = s - hy_ref[0:1, cols]
            for h in range(deep // LANES):
                at = r * deep + h * LANES
                sub = slice(at, at + LANES)
                top = s_ref[sub, 0:LANES]
                for l in range(1, nl):
                    top = jnp.maximum(top, s_ref[sub, l * LANES : (l + 1) * LANES])
                peak = jnp.broadcast_to(jnp.max(top, 1, keepdims=True), (LANES, LANES))
                acc = jnp.zeros((LANES, LANES), F32)
                for l in range(nl):
                    acc = acc + jnp.exp2(s_ref[sub, l * LANES : (l + 1) * LANES] - peak)
                stat_ref[0:1, sub] = jnp.max(top.T, 0, keepdims=True)
                stat_ref[1:2, sub] = jnp.sum(acc.T, 0, keepdims=True)

    cross = pl.pallas_call(
        cross_body,
        in_specs=[pl.BlockSpec(memory_space=pltpu.SMEM)] + [pl.BlockSpec(memory_space=pltpu.VMEM)] * (2 + A * Y),
        out_shape=(
            sds((M, N), F32), sds((M, F), F32), sds((F, N), BF16), sds((F, N), BF16),
            sds((1, N), F32), sds((3, M), F32), sds((1, N), F32), sds((2, M), F32),
        ),
        scratch_shapes=(
            pltpu.VMEM((F, M), F32), pltpu.VMEM((F, N), F32), pltpu.VMEM((M, F), BF16), pltpu.VMEM((M, F), BF16),
        ),
        compiler_params=pltpu.CompilerParams(vmem_limit_bytes=36 * MB),
    )

    def fill_cols(col_ref, row):
        for r in range(nr):
            sub = slice(r * LANES, (r + 1) * LANES)
            col_ref[sub, :] = to_col(row[:, sub])

    def online(v, l, m_ref, e_ref):
        lane = slice(l * LANES, (l + 1) * LANES)
        g = groups(v)
        old = m_ref[:, lane]
        new = jnp.maximum(old, jnp.max(g, 0))
        e_ref[:, lane] = e_ref[:, lane] * jnp.exp2(old - new) + jnp.sum(jnp.exp2(g - new[None]), 0)
        m_ref[:, lane] = new

    def finish(m_ref, e_ref, out_ref):
        m = m_ref[...]
        top = jnp.max(m, 0, keepdims=True)
        out_ref[0:1, :] = top
        out_ref[1:2, :] = jnp.sum(e_ref[...] * jnp.exp2(m - top), 0, keepdims=True)

    def start(m_ref, e_ref):
        m_ref[...] = jnp.full((8, N), -1e30, F32)
        e_ref[...] = jnp.zeros((8, N), F32)

    def col1_body(s_ref, stat, rowc, f_ref, out_ref, col_ref, m_ref, e_ref):
        f = rowc[0:1, :] * LOG2E - (stat[0:1, :] + log2(stat[1:2, :]))
        f_ref[...] = f
        fill_cols(col_ref, f)
        start(m_ref, e_ref)

        @pl.loop(0, nr)
        def _(r):
            rows = pl.ds(pl.multiple_of(r * LANES, LANES), LANES)
            fc = col_ref[rows, :]
            for l in range(nl):
                online(s_ref[rows, l * LANES : (l + 1) * LANES] + fc, l, m_ref, e_ref)

        finish(m_ref, e_ref, out_ref)

    stats = (pltpu.VMEM((M, LANES), F32), pltpu.VMEM((8, N), F32), pltpu.VMEM((8, N), F32))
    col1 = call(col1_body, (sds((1, M), F32), sds((2, N), F32)), stats, 14)

    def row2_body(s_ref, f, stat, logb, g_ref, out_ref, col_ref):
        g_ref[...] = logb[...] * LOG2E - (stat[0:1, :] + log2(stat[1:2, :]))
        fill_cols(col_ref, f)

        for r in range(nr):
            rows = slice(r * LANES, (r + 1) * LANES)
            fc = col_ref[rows, :]
            acc = jnp.zeros((LANES, LANES), F32)
            for l in range(nl):
                lane = slice(l * LANES, (l + 1) * LANES)
                acc = acc + jnp.exp2(s_ref[rows, lane] + fc + g_ref[:, lane])
            out_ref[0:1, rows] = jnp.sum(acc.T, 0, keepdims=True)

    row2 = call(row2_body, (sds((1, N), F32), sds((1, M), F32)), (stats[0],), 14)

    def col2_body(s_ref, f, g, total, rowc, f_ref, out_ref, col_ref, acc_ref):
        f2 = f[...] + rowc[0:1, :] * LOG2E - log2(total[...])
        f_ref[...] = f2
        fill_cols(col_ref, f2)
        acc_ref[...] = jnp.zeros((8, N), F32)

        @pl.loop(0, nr)
        def _(r):
            rows = pl.ds(pl.multiple_of(r * LANES, LANES), LANES)
            fc = col_ref[rows, :]
            for l in range(nl):
                lane = slice(l * LANES, (l + 1) * LANES)
                p = jnp.exp2(s_ref[rows, lane] + fc + g[:, lane])
                acc_ref[:, lane] = acc_ref[:, lane] + jnp.sum(groups(p), 0)

        out_ref[...] = jnp.sum(acc_ref[...], 0, keepdims=True)

    col2 = call(col2_body, (sds((1, M), F32), sds((1, N), F32)), stats[:2], 14)

    nm = pb // F if pb >= F else 1
    mw = min(pb, F)

    def plan_body(s_ref, f, g, total, logb, yh, yl, w_ref, col_ref, g_ref, ph_ref, pl_ref):
        g_ref[...] = g[...] + logb[...] * LOG2E - log2(total[...])
        fill_cols(col_ref, f)
        for r in range(nr):
            rows = slice(r * LANES, (r + 1) * LANES)
            fc = col_ref[rows, :]
            acc = jnp.zeros((LANES, LANES), F32)
            for l in range(nl):
                lane = slice(l * LANES, (l + 1) * LANES)
                p = jnp.exp2(s_ref[rows, lane] + fc + g_ref[:, lane])
                acc = acc + p
                ph_ref[rows, lane], pl_ref[rows, lane] = split(p)
            mass = jnp.sum(acc.T, 0, keepdims=True)
            h, at = divmod(r * LANES, pb)
            w_ref[h, pb + at // mw : pb + at // mw + 1, at % mw : at % mw + LANES] = mass
            w_ref[h, at : at + LANES, :] = dot3(
                ph_ref[rows, :], pl_ref[rows, :], yh[...], yl[...], ((1,), (1,))
            )

    plan = call(
        plan_body,
        sds((2, pb + 8, F), F32),
        (stats[0], pltpu.VMEM((1, N), F32), pltpu.VMEM((M, N), BF16), pltpu.VMEM((M, N), BF16)),
        36,
    )

    def last_body(place, own, other, xt, f, rowc, yh, yl, hy, mt_ref, f_ref, out_ref, s_ref, m_ref, e_ref):
        c = place[1]
        f_ref[...] = (EPS * LN2) * (f[...] + rowc[2:3, :])
        start(m_ref, e_ref)
        deep = min(256, pb)
        wide = 512
        for r in range(M // deep):
            for h in range(deep // LANES):
                at = r * deep + h * LANES
                half_of, inner = divmod(at, pb)
                rows = slice(at, at + LANES)
                pick = lambda i, j, n, m: jnp.where(
                    c == half_of, own[i : i + n, j : j + m], other[i : i + n, j : j + m]
                )
                mass = pick(pb + inner // mw, inner % mw, 1, LANES)
                t = rowc[1:2, rows]
                keep = jnp.tile(to_col(1.0 - t), (1, F // LANES))
                take = jnp.tile(to_col(t / mass), (1, F // LANES))
                mv = keep * xt[rows, :] + take * pick(inner, 0, LANES, F)
                mt = mv.T
                mt_ref[:, rows] = mt
                nm_row = (0.5 * L) * jnp.sum(mt * mt, 0, keepdims=True)
                fc = to_col(f[:, rows] + rowc[2:3, rows] - nm_row)
                mh, ml = split(mv * L)
                for j in range(N // wide):
                    cols = slice(j * wide, (j + 1) * wide)
                    v = dot3(mh, ml, yh[:, cols], yl[:, cols], ((1,), (0,))) - hy[0:1, cols]
                    for l in range(wide // LANES):
                        lane = slice(l * LANES, (l + 1) * LANES)
                        online(v[:, lane] + fc, j * (wide // LANES) + l, m_ref, e_ref)
        finish(m_ref, e_ref, out_ref)

    last = pl.pallas_call(
        last_body,
        in_specs=[pl.BlockSpec(memory_space=pltpu.SMEM)] + [pl.BlockSpec(memory_space=pltpu.VMEM)] * 8,
        out_shape=(sds((F, M), F32), sds((1, M), F32), sds((2, N), F32)),
        scratch_shapes=(pltpu.VMEM((8, LANES), F32), stats[1], stats[2]),
        compiler_params=pltpu.CompilerParams(vmem_limit_bytes=24 * MB),
    )
    return cross, col1, row2, col2, plan, last


def solution(mesh):
    S, T = mesh.shape["src"], mesh.shape["tgt"]
    Y, A = S // 2, T // 2

    def swap(v, axis, size, k):
        return lax.ppermute(v, axis, [(i, i ^ k) for i in range(size)])

    def over_c(v):
        return swap(v, "src", S, 1)

    def over_y(v, k):
        return swap(v, "src", S, 2 * k)

    def over_b(v):
        return swap(v, "tgt", T, 1)

    def over_a(v, k):
        return swap(v, "tgt", T, 2 * k)

    def join(p, q):
        top = jnp.maximum(p[0:1], q[0:1])
        return jnp.concatenate([top, p[1:2] * jnp.exp2(p[0:1] - top) + q[1:2] * jnp.exp2(q[0:1] - top)])

    def add(p, q):
        return p + q

    def merge_rows(v, op):
        v = op(v, over_c(v))
        return op(v, over_b(v))

    def merge_y(v, op):
        k = 1
        while k < Y:
            v = op(v, over_y(v, k))
            k *= 2
        return v

    def merge_cols(v, op):
        v = merge_y(v, op)
        k = 1
        while k < A:
            v = op(v, over_a(v, k))
            k *= 2
        return v

    def per_device(sources, targets, source_logw, target_logw, times):
        ft, ns = sources.shape
        fs, nt = targets.shape
        F = ft * T
        half, pb = nt // 2, ns // A
        M, N = 2 * pb, A * half
        s, t = lax.axis_index("src"), lax.axis_index("tgt")
        y, c, a, b = s // 2, s % 2, t // 2, t % 2
        place = jnp.stack([y, c, a, b]).astype(jnp.int32)
        cross, col1, row2, col2, plan, last = kernels(F, M, N, fs, ft, A, Y, half, pb)

        kept = lax.dynamic_slice(targets, (0, c * half), (fs, half))
        sent = lax.dynamic_slice(targets, (0, (1 - c) * half), (fs, half))
        logb_mine = lax.dynamic_slice(target_logw, (c * half,), (half,))[None]
        own = jnp.concatenate([kept, over_c(sent), jnp.broadcast_to(logb_mine, (8, half))])
        chunks = [own] + [over_a(own, k) for k in range(1, A)]
        pieces = []
        for ch in chunks:
            pieces += [ch] + [over_y(ch, m) for m in range(1, Y)]

        def block(k):
            return lax.dynamic_slice(sources, (0, (a ^ k) * pb), (ft, pb))

        xs = jnp.concatenate([block(0)] + [over_a(block(k), k) for k in range(1, A)])
        side = jnp.stack([source_logw, times])
        side = jnp.pad(lax.dynamic_slice(side, (0, a * pb), (2, pb)), ((0, 6), (0, 0)))
        x_own = jnp.concatenate([xs, over_b(xs), side])
        x_other = over_c(x_own)

        sc, xt, yh, yl, hy, rowc, logb, stat = cross(place, x_own, x_other, *pieces)
        stat = merge_rows(stat, join)
        f1, stat = col1(sc, stat, rowc)
        stat = merge_cols(stat, join)
        g1, total = row2(sc, f1, stat, logb)
        total = merge_rows(total, add)
        f2, total = col2(sc, f1, g1, total, rowc)
        total = merge_cols(total, add)
        w = plan(sc, f2, g1, total, logb, yh, yl)
        mine = lax.dynamic_index_in_dim(w, c, 0, keepdims=False)
        theirs = lax.dynamic_index_in_dim(w, 1 - c, 0, keepdims=False)
        mine = mine + over_c(theirs)
        mine = mine + over_b(mine)
        moved_t, f_out, stat = last(place, mine, over_c(mine), xt, f2, rowc, yh, yl, hy)

        stat = merge_y(stat, join)

        def parcel(k):
            at = a ^ k
            feats = lax.dynamic_slice(moved_t, ((at * 2 + b) * ft, c * pb), (ft, pb))
            pot = lax.dynamic_slice(f_out, (0, c * pb), (1, pb))
            return jnp.concatenate([feats, pot, lax.dynamic_slice(stat, (0, at * half), (2, half)).reshape(-1, pb)])

        moved = jnp.zeros((ft, ns), F32)
        row_pot = jnp.zeros((1, ns), F32)
        col = None
        for k in range(A):
            got = parcel(k) if k == 0 else over_a(parcel(k), k)
            at = (a ^ k) * pb
            moved = lax.dynamic_update_slice(moved, got[:ft], (0, at))
            row_pot = lax.dynamic_update_slice(row_pot, got[ft : ft + 1], (0, at))
            part = got[ft + 1 :].reshape(2, half)
            col = part if col is None else join(col, part)
        pot = EPS * (logb_mine - LN2 * (col[0:1] + log2(col[1:2])))
        far = over_c(pot)
        col_pot = jnp.concatenate([jnp.where(c == 0, pot, far), jnp.where(c == 0, far, pot)], 1)
        return row_pot[0], moved, col_pot[0]

    placed = (P("tgt", "src"), P("src", "tgt"), P("src"), P("tgt"), P("src"))
    return jax.shard_map(
        per_device,
        mesh=mesh,
        in_specs=placed,
        out_specs=(P("src"), P("tgt", "src"), P("tgt")),
        check_vma=False,
    )
```

```python
import jax
import jax.numpy as jnp
from jax import lax
from jax.experimental import pallas as pl
from jax.experimental.pallas import tpu as pltpu
from jax.sharding import PartitionSpec as P


EPS = 16.0
LOG2E = 1.4426950408889634
LN2 = 0.6931471805599453
L = LOG2E / EPS
LANES = 128
F32 = jnp.float32
BF16 = jnp.bfloat16
MB = 1024 * 1024


def split(v):
    hi = v.astype(BF16)
    return hi, (v - hi.astype(F32)).astype(BF16)


def dot3(ah, al, bh, bl, dims):
    d = lambda p, q: lax.dot_general(p, q, (dims, ((), ())), preferred_element_type=F32)
    return d(ah, bh) + d(ah, bl) + d(al, bh)


def to_col(row):
    return jnp.broadcast_to(row, (LANES, LANES)).T


def log2(v):
    return jnp.log(v) * LOG2E


def groups(v):
    return v.reshape(v.shape[0] // 8, 8, v.shape[1])


def call(body, outs, scratch, limit):
    return pl.pallas_call(
        body,
        out_shape=outs,
        scratch_shapes=scratch,
        compiler_params=pltpu.CompilerParams(vmem_limit_bytes=limit * MB),
    )


def sds(*shape, dtype=F32):
    return jax.ShapeDtypeStruct(shape, dtype)


def position():
    s, t = lax.axis_index("src"), lax.axis_index("tgt")
    return s >> 1, s & 1, t >> 1, t & 1


def lanes_at(index, size):
    return pl.ds(pl.multiple_of(index * size, LANES), size)


def rows_at(index, size):
    return pl.ds(pl.multiple_of(index * size, 8), size)


def joined(p, q):
    top = jnp.maximum(p[0:1, :], q[0:1, :])
    return top, p[1:2, :] * jnp.exp2(p[0:1, :] - top) + q[1:2, :] * jnp.exp2(q[0:1, :] - top)


def lse2(p, q):
    top, total = joined(p, q)
    return top + log2(total)


class Kernels:
    def __init__(self, F, fs, ft, A, Y, half, pb, Q):
        self.F, self.fs, self.ft, self.A, self.Y, self.half, self.pb, self.Q = F, fs, ft, A, Y, half, pb, Q
        self.M, self.N = 2 * pb, A * half
        self.nl, self.nr = self.N // LANES, self.M // LANES
        self.qr = pb // Q
        self.mw = min(self.qr, F)
        self.hw = min(half, pb)

    def prep(self, sources, targets, source_logw, target_logw, times):
        fs, ft, A, half, pb = self.fs, self.ft, self.A, self.half, self.pb

        def body(x, v, la, lb, tm, sent, kept, *rest):
            blocks, side = rest[:A], rest[A]
            _, c, a, _ = position()
            sent[...] = v[:, lanes_at(1 - c, half)]
            kept[0:fs, :] = v[:, lanes_at(c, half)]
            kept[fs : fs + 8, :] = jnp.broadcast_to(lb[0:1, lanes_at(c, half)], (8, half))
            for k in range(A):
                blocks[k][...] = x[:, lanes_at(a ^ k, pb)]
            side[0:4, :] = jnp.broadcast_to(la[0:1, lanes_at(a, pb)], (4, pb))
            side[4:8, :] = jnp.broadcast_to(tm[0:1, lanes_at(a, pb)], (4, pb))

        outs = (sds(fs, half), sds(fs + 8, half), *(sds(ft, pb) for _ in range(A)), sds(8, pb))
        out = call(body, outs, (), 8)(sources, targets, source_logw[None], target_logw[None], times[None])
        return out[0], out[1], out[2 : 2 + A], out[2 + A]

    def cross(self, own, other, pieces):
        F, M, N, A, Y, fs, ft, half, pb, nl = (
            self.F, self.M, self.N, self.A, self.Y, self.fs, self.ft, self.half, self.pb, self.nl,
        )

        def body(own, other, *refs):
            pieces = refs[: A * Y]
            s_ref, xt_ref, yh_ref, yl_ref, hy_ref, rowc_ref, logb_ref, stat_ref = refs[A * Y : A * Y + 8]
            x_ref, y_ref, xh_ref, xl_ref = refs[A * Y + 8 :]
            y, c, a, b = position()
            for k in range(A):
                for q in range(2):
                    at = rows_at((a ^ k) * 2 + (b ^ q), ft)
                    src = slice((q * A + k) * ft, (q * A + k + 1) * ft)
                    x_ref[at, lanes_at(c, pb)] = own[src, :]
                    x_ref[at, lanes_at(1 - c, pb)] = other[src, :]
            for row in range(2):
                rowc_ref[row : row + 1, lanes_at(c, pb)] = own[F + 4 * row : F + 4 * row + 1, :]
                rowc_ref[row : row + 1, lanes_at(1 - c, pb)] = other[F + 4 * row : F + 4 * row + 1, :]
            for k in range(A):
                cols = lanes_at(a ^ k, half)
                for m in range(Y):
                    p = pieces[k * Y + m]
                    y_ref[rows_at((y ^ m) * 2 + c, fs), cols] = p[0:fs, :]
                    y_ref[rows_at((y ^ m) * 2 + (1 - c), fs), cols] = p[fs + 8 : 2 * fs + 8, :]
                logb_ref[0:1, cols] = pieces[k * Y][fs : fs + 1, :]
            for j in range(N // 256):
                cols = slice(j * 256, (j + 1) * 256)
                v = y_ref[:, cols]
                hy_ref[0:1, cols] = (0.5 * L) * jnp.sum(v * v, 0, keepdims=True)
                yh_ref[:, cols], yl_ref[:, cols] = split(v)
            for r in range(self.nr):
                rows = slice(r * LANES, (r + 1) * LANES)
                v = x_ref[:, rows]
                rowc_ref[2:3, rows] = (0.5 * L) * jnp.sum(v * v, 0, keepdims=True)
                vt = v.T
                xt_ref[rows, :] = vt
                xh_ref[rows, :], xl_ref[rows, :] = split(vt * L)
            wide = 512
            deep = min(256, M)
            for r in range(M // deep):
                rows = slice(r * deep, (r + 1) * deep)
                for j in range(N // wide):
                    cols = slice(j * wide, (j + 1) * wide)
                    s = dot3(xh_ref[rows, :], xl_ref[rows, :], yh_ref[:, cols], yl_ref[:, cols], ((1,), (0,)))
                    s_ref[rows, cols] = s - hy_ref[0:1, cols]
                for h in range(deep // LANES):
                    at = r * deep + h * LANES
                    sub = slice(at, at + LANES)
                    top = s_ref[sub, 0:LANES]
                    for l in range(1, nl):
                        top = jnp.maximum(top, s_ref[sub, l * LANES : (l + 1) * LANES])
                    peak = jnp.broadcast_to(jnp.max(top, 1, keepdims=True), (LANES, LANES))
                    acc = jnp.zeros((LANES, LANES), F32)
                    for l in range(nl):
                        acc = acc + jnp.exp2(s_ref[sub, l * LANES : (l + 1) * LANES] - peak)
                    stat_ref[0:1, sub] = jnp.max(top.T, 0, keepdims=True)
                    stat_ref[1:2, sub] = jnp.sum(acc.T, 0, keepdims=True)

        outs = (
            sds(M, N), sds(M, F), sds(F, N, dtype=BF16), sds(F, N, dtype=BF16), sds(1, N), sds(3, M), sds(1, N), sds(2, M),
        )
        scratch = (pltpu.VMEM((F, M), F32), pltpu.VMEM((F, N), F32), pltpu.VMEM((M, F), BF16), pltpu.VMEM((M, F), BF16))
        return call(body, outs, scratch, 20)(own, other, *pieces)

    def fill_cols(self, col_ref, row):
        for r in range(self.nr):
            sub = slice(r * LANES, (r + 1) * LANES)
            col_ref[sub, :] = to_col(row[:, sub])

    def online(self, v, l, m_ref, e_ref):
        lane = slice(l * LANES, (l + 1) * LANES)
        g = groups(v)
        old = m_ref[:, lane]
        new = jnp.maximum(old, jnp.max(g, 0))
        e_ref[:, lane] = e_ref[:, lane] * jnp.exp2(old - new) + jnp.sum(jnp.exp2(g - new[None]), 0)
        m_ref[:, lane] = new

    def finish(self, m_ref, e_ref, out_ref):
        m = m_ref[...]
        top = jnp.max(m, 0, keepdims=True)
        out_ref[0:1, :] = top
        out_ref[1:2, :] = jnp.sum(e_ref[...] * jnp.exp2(m - top), 0, keepdims=True)

    def start(self, m_ref, e_ref):
        m_ref[...] = jnp.full((8, self.N), -1e30, F32)
        e_ref[...] = jnp.zeros((8, self.N), F32)

    def stats(self):
        return pltpu.VMEM((8, self.N), F32), pltpu.VMEM((8, self.N), F32)

    def cols(self):
        return pltpu.VMEM((self.M, LANES), F32)

    def col1(self, s, stat, far, rowc):
        def body(s_ref, stat, far, rowc, f_ref, out_ref, col_ref, m_ref, e_ref):
            f = rowc[0:1, :] * LOG2E - lse2(stat, far)
            f_ref[...] = f
            self.fill_cols(col_ref, f)
            self.start(m_ref, e_ref)

            @pl.loop(0, self.nr)
            def _(r):
                rows = pl.ds(pl.multiple_of(r * LANES, LANES), LANES)
                fc = col_ref[rows, :]
                for l in range(self.nl):
                    self.online(s_ref[rows, l * LANES : (l + 1) * LANES] + fc, l, m_ref, e_ref)

            self.finish(m_ref, e_ref, out_ref)

        return call(body, (sds(1, self.M), sds(2, self.N)), (self.cols(), *self.stats()), 10)(s, stat, far, rowc)

    def row2(self, s, f, stat, far, logb):
        def body(s_ref, f, stat, far, logb, g_ref, out_ref, col_ref):
            g_ref[...] = logb[...] * LOG2E - lse2(stat, far)
            self.fill_cols(col_ref, f)
            for r in range(self.nr):
                rows = slice(r * LANES, (r + 1) * LANES)
                fc = col_ref[rows, :]
                acc = jnp.zeros((LANES, LANES), F32)
                for l in range(self.nl):
                    lane = slice(l * LANES, (l + 1) * LANES)
                    acc = acc + jnp.exp2(s_ref[rows, lane] + fc + g_ref[:, lane])
                out_ref[0:1, rows] = jnp.sum(acc.T, 0, keepdims=True)

        return call(body, (sds(1, self.N), sds(1, self.M)), (self.cols(),), 10)(s, f, stat, far, logb)

    def col2(self, s, f, g, total, far, rowc):
        def body(s_ref, f, g, total, far, rowc, f_ref, out_ref, col_ref, acc_ref):
            f2 = f[...] + rowc[0:1, :] * LOG2E - log2(total[...] + far[...])
            f_ref[...] = f2
            self.fill_cols(col_ref, f2)
            acc_ref[...] = jnp.zeros((8, self.N), F32)

            @pl.loop(0, self.nr)
            def _(r):
                rows = pl.ds(pl.multiple_of(r * LANES, LANES), LANES)
                fc = col_ref[rows, :]
                for l in range(self.nl):
                    lane = slice(l * LANES, (l + 1) * LANES)
                    p = jnp.exp2(s_ref[rows, lane] + fc + g[:, lane])
                    acc_ref[:, lane] = acc_ref[:, lane] + jnp.sum(groups(p), 0)

            out_ref[...] = jnp.sum(acc_ref[...], 0, keepdims=True)

        scratch = (self.cols(), self.stats()[0])
        return call(body, (sds(1, self.M), sds(1, self.N)), scratch, 10)(s, f, g, total, far, rowc)

    def plan(self, s, f, g, total, far, logb, yh, yl, mine, q, base):
        N, F, qr, mw = self.N, self.F, self.qr, self.mw

        def body(s_ref, f, g, total, far, logb, yh, yl, *rest):
            extra, (w_ref, g_ref, ph_ref, pl_ref) = rest[:-4], rest[-4:]
            _, c, _, _ = position()
            at = (c if mine else 1 - c) * self.pb + q * qr
            g_ref[...] = g[...] + logb[...] * LOG2E - log2(total[...] + far[...])
            for r in range(qr // LANES):
                fc = to_col(f[0:1, pl.ds(pl.multiple_of(at + r * LANES, LANES), LANES)])
                rows = pl.ds(pl.multiple_of(at + r * LANES, LANES), LANES)
                local = slice(r * LANES, (r + 1) * LANES)
                acc = jnp.zeros((LANES, LANES), F32)
                for l in range(self.nl):
                    lane = slice(l * LANES, (l + 1) * LANES)
                    p = jnp.exp2(s_ref[rows, lane] + fc + g_ref[:, lane])
                    acc = acc + p
                    ph_ref[local, lane], pl_ref[local, lane] = split(p)
                i, j = divmod(r * LANES, mw)
                mass = jnp.sum(acc.T, 0, keepdims=True)
                if extra:
                    mass = mass + extra[0][qr + i : qr + i + 1, j : j + LANES]
                w_ref[qr + i : qr + i + 1, j : j + LANES] = mass
            w = dot3(ph_ref[...], pl_ref[...], yh[...], yl[...], ((1,), (1,)))
            w_ref[0:qr, :] = w + extra[0][0:qr, :] if extra else w

        scratch = (pltpu.VMEM((1, N), F32), pltpu.VMEM((qr, N), BF16), pltpu.VMEM((qr, N), BF16))
        args = (s, f, g, total, far, logb, yh, yl) + (() if base is None else (base,))
        return call(body, sds(qr + 8, F), scratch, 14)(*args)

    def last(self, own, other, xt, f, rowc, yh, yl, hy, q):
        F, M, N, A, ft, pb, qr, mw = self.F, self.M, self.N, self.A, self.ft, self.pb, self.qr, self.mw

        def entry(*refs):
            ins, outs, (m_ref, e_ref, mt_ref) = refs[:8], refs[8:-3], refs[-3:]
            parcels, out_ref = outs[:A], outs[A]
            body(*ins, parcels, out_ref, m_ref, e_ref, mt_ref)

        def body(own, other, xt, f, rowc, yh, yl, hy, parcels, out_ref, m_ref, e_ref, mt_ref):
            _, c, a, b = position()
            self.start(m_ref, e_ref)
            wide = min(512, N)
            for src, core in ((own, c), (other, 1 - c)):
                for r in range(qr // LANES):
                    at = pl.ds(pl.multiple_of(core * pb + (q * qr + r * LANES), LANES), LANES)
                    i, j = divmod(r * LANES, mw)
                    t = rowc[1:2, at]
                    nx = rowc[2:3, at]
                    keep = jnp.tile(to_col(1.0 - t), (1, F // LANES))
                    take = jnp.tile(to_col(t / src[qr + i : qr + i + 1, j : j + LANES]), (1, F // LANES))
                    mv = keep * xt[at, :] + take * src[r * LANES : (r + 1) * LANES, :]
                    mt = mv.T
                    if src is own:
                        lane = slice(r * LANES, (r + 1) * LANES)
                        mt_ref[:, lane] = mt
                        for k in range(A):
                            parcels[k][ft : ft + 8, lane] = jnp.broadcast_to((EPS * LN2) * (f[0:1, at] + nx), (8, LANES))
                    fc = to_col(f[0:1, at] + nx - (0.5 * L) * jnp.sum(mt * mt, 0, keepdims=True))
                    mh, ml = split(mv * L)
                    for n in range(N // wide):
                        cols = slice(n * wide, (n + 1) * wide)
                        v = dot3(mh, ml, yh[:, cols], yl[:, cols], ((1,), (0,))) - hy[0:1, cols]
                        for l in range(wide // LANES):
                            lane = slice(l * LANES, (l + 1) * LANES)
                            self.online(v[:, lane] + fc, n * (wide // LANES) + l, m_ref, e_ref)
            for k in range(A):
                parcels[k][0:ft, :] = mt_ref[rows_at((a ^ k) * 2 + b, ft), :]
            self.finish(m_ref, e_ref, out_ref)

        outs = (*(sds(ft + 8, qr) for _ in range(A)), sds(2, N))
        out = call(entry, outs, (*self.stats(), pltpu.VMEM((F, qr), F32)), 14)(own, other, xt, f, rowc, yh, yl, hy)
        return out[:A], out[A]

    def pack(self, parcels, stat, far):
        A, Q, ft, qr, pb, half, hw = self.A, self.Q, self.ft, self.qr, self.pb, self.half, self.hw

        def body(*refs):
            parts, (p, q), outs, st = refs[: A * Q], refs[A * Q : A * Q + 2], refs[A * Q + 2 : -1], refs[-1]
            _, _, a, _ = position()
            st[0:1, :], st[1:2, :] = joined(p, q)
            for k in range(A):
                for i in range(Q):
                    outs[k][:, i * qr : (i + 1) * qr] = parts[i * A + k][...]
                for i in range(half // hw):
                    at = pl.ds(pl.multiple_of((a ^ k) * half + i * hw, LANES), hw)
                    outs[k][ft + 1 + 2 * i : ft + 3 + 2 * i, 0:hw] = st[0:2, at]

        outs = tuple(sds(ft + 8, pb) for _ in range(A))
        flat = [p for part in parcels for p in part]
        return call(body, outs, (pltpu.VMEM((2, self.N), F32),), 8)(*flat, stat, far)

    def unpack(self, got, kept):
        A, fs, ft, pb, half, hw = self.A, self.fs, self.ft, self.pb, self.half, self.hw

        def body(*refs):
            got, kept, moved, row_pot, pot = refs[:A], refs[A], refs[A + 1], refs[A + 2], refs[A + 3]
            _, _, a, _ = position()
            for k in range(A):
                cols = lanes_at(a ^ k, pb)
                moved[:, cols] = got[k][0:ft, :]
                row_pot[0:1, cols] = got[k][ft : ft + 1, :]
            for i in range(half // hw):
                tops = [got[k][ft + 1 + 2 * i : ft + 2 + 2 * i, 0:hw] for k in range(A)]
                top = tops[0]
                for v in tops[1:]:
                    top = jnp.maximum(top, v)
                total = jnp.zeros_like(top)
                for k in range(A):
                    total = total + got[k][ft + 2 + 2 * i : ft + 3 + 2 * i, 0:hw] * jnp.exp2(tops[k] - top)
                lanes = slice(i * hw, (i + 1) * hw)
                pot[0:1, lanes] = EPS * (kept[fs : fs + 1, lanes] - LN2 * (top + log2(total)))

        return call(body, (sds(ft, A * pb), sds(1, A * pb), sds(1, half)), (), 8)(*got, kept)

    def pair(self, pot, far):
        def body(p, q, out):
            _, c, _, _ = position()
            out[0:1, lanes_at(c, self.half)] = p[...]
            out[0:1, lanes_at(1 - c, self.half)] = q[...]

        return call(body, sds(1, 2 * self.half), (), 8)(pot, far)


def solution(mesh):
    S, T = mesh.shape["src"], mesh.shape["tgt"]
    Y, A = S // 2, T // 2

    def swap(v, axis, size, k):
        return lax.ppermute(v, axis, [(i, i ^ k) for i in range(size)])

    def over_c(v):
        return swap(v, "src", S, 1)

    def over_y(v, k):
        return swap(v, "src", S, 2 * k)

    def over_b(v):
        return swap(v, "tgt", T, 1)

    def over_a(v, k):
        return swap(v, "tgt", T, 2 * k)

    def join(p, q):
        return jnp.concatenate(joined(p, q))

    def add(p, q):
        return p + q

    def last_two(v, op, sends):
        for send in sends[:-1]:
            v = op(v, send(v))
        return v, sends[-1](v)

    def bits(size):
        return [1 << i for i in range(size.bit_length() - 1)]

    over_rows = [over_c, over_b]
    along_y = [lambda v, k=k: over_y(v, k) for k in bits(Y)]
    over_cols = along_y + [lambda v, k=k: over_a(v, k) for k in bits(A)]

    def per_device(sources, targets, source_logw, target_logw, times):
        ft, ns = sources.shape
        fs, nt = targets.shape
        half, pb = nt // 2, ns // A
        Q = 2 if pb % 256 == 0 else 1
        kern = Kernels(ft * T, fs, ft, A, Y, half, pb, Q)

        sent, kept, blocks, side = kern.prep(sources, targets, source_logw, target_logw, times)
        own = jnp.concatenate([kept, over_c(sent)])
        chunks = {0: own}
        for bit in reversed(bits(A)):
            for k in list(chunks):
                chunks[k ^ bit] = over_a(chunks[k], bit)
        pieces = []
        for k in range(A):
            pieces.append(chunks[k])
            for m in range(1, Y):
                pieces.append(over_y(chunks[k], m))
        parts = [blocks[0]]
        for k in range(1, A):
            parts.append(over_a(blocks[k], k))
        xs = jnp.concatenate(parts)
        xb = over_b(xs)
        x_own = jnp.concatenate([xs, xb, side])
        x_other = over_c(x_own)

        sc, xt, yh, yl, hy, rowc, logb, stat = kern.cross(x_own, x_other, pieces)
        f1, stat = kern.col1(sc, *last_two(stat, join, over_rows), rowc)
        g1, total = kern.row2(sc, f1, *last_two(stat, join, over_cols), logb)
        f2, total = kern.col2(sc, f1, g1, *last_two(total, add, over_rows), rowc)
        total = last_two(total, add, over_cols)

        def plan(mine, q, base):
            return kern.plan(sc, f2, g1, *total, logb, yh, yl, mine, q, base)

        theirs = [over_c(plan(False, q, None)) for q in range(Q)]
        parcels, stat = [], None
        for q in range(Q):
            w = plan(True, q, theirs[q])
            w = w + over_b(w)
            part, fresh = kern.last(w, over_c(w), xt, f2, rowc, yh, yl, hy, q)
            parcels.append(part)
            stat = fresh if stat is None else join(stat, fresh)

        packed = kern.pack(parcels, *last_two(stat, join, along_y))
        got = [packed[0]] + [over_a(packed[k], k) for k in range(1, A)]
        moved, row_pot, pot = kern.unpack(got, kept)
        col_pot = kern.pair(pot, over_c(pot))
        return row_pot[0], moved, col_pot[0]

    placed = (P("tgt", "src"), P("src", "tgt"), P("src"), P("tgt"), P("src"))
    return jax.shard_map(
        per_device,
        mesh=mesh,
        in_specs=placed,
        out_specs=(P("src"), P("tgt", "src"), P("tgt")),
        check_vma=False,
    )
```

```python
import jax
import jax.numpy as jnp
from jax import lax
from jax.experimental import pallas as pl
from jax.experimental.pallas import tpu as pltpu
from jax.sharding import PartitionSpec as P


EPS = 16.0
LOG2E = 1.4426950408889634
LN2 = 0.6931471805599453
L = LOG2E / EPS
LANES = 128
F32 = jnp.float32
BF16 = jnp.bfloat16
MB = 1024 * 1024


def split(v):
    hi = v.astype(BF16)
    return hi, (v - hi.astype(F32)).astype(BF16)


def dot3(ah, al, bh, bl, dims):
    d = lambda p, q: lax.dot_general(p, q, (dims, ((), ())), preferred_element_type=F32)
    return d(ah, bh) + d(ah, bl) + d(al, bh)


def to_col(row):
    return jnp.broadcast_to(row, (LANES, LANES)).T


def log2(v):
    return jnp.log(v) * LOG2E


def groups(v):
    return v.reshape(v.shape[0] // 8, 8, v.shape[1])


def call(body, outs, scratch, limit):
    return pl.pallas_call(
        body,
        out_shape=outs,
        scratch_shapes=scratch,
        compiler_params=pltpu.CompilerParams(vmem_limit_bytes=limit * MB),
    )


def sds(*shape, dtype=F32):
    return jax.ShapeDtypeStruct(shape, dtype)


def position():
    s, t = lax.axis_index("src"), lax.axis_index("tgt")
    return s >> 1, s & 1, t >> 1, t & 1


def lanes_at(index, size):
    return pl.ds(pl.multiple_of(index * size, LANES), size)


def rows_at(index, size):
    return pl.ds(pl.multiple_of(index * size, 8), size)


def joined(values):
    top = values[0][0:1, :]
    for v in values[1:]:
        top = jnp.maximum(top, v[0:1, :])
    return top, total([v[1:2, :] * jnp.exp2(v[0:1, :] - top) for v in values])


def total(values):
    acc = values[0][...]
    for v in values[1:]:
        acc = acc + v[...]
    return acc


def lse2(values):
    top, acc = joined(values)
    return top + log2(acc)


class Kernels:
    def __init__(self, F, fs, ft, A, Y, half, pb, Q):
        self.F, self.fs, self.ft, self.A, self.Y, self.half, self.pb, self.Q = F, fs, ft, A, Y, half, pb, Q
        self.M, self.N = 2 * pb, A * half
        self.nl, self.nr = self.N // LANES, self.M // LANES
        self.qr = pb // Q
        self.mw = min(self.qr, F)
        self.hw = min(half, self.qr)
        self.tail = -(-(1 + 2 * (half // self.hw)) // 8) * 8

    def prep(self, sources, targets, source_logw, target_logw, times):
        fs, ft, A, half, pb = self.fs, self.ft, self.A, self.half, self.pb

        def body(x, v, la, lb, tm, sent, kept, *rest):
            blocks, side, row, sems = rest[:A], rest[A], rest[A + 1], rest[A + 2]
            _, c, a, _ = position()
            pairs = [
                (v.at[:, lanes_at(1 - c, half)], sent),
                (v.at[:, lanes_at(c, half)], kept.at[0:fs, :]),
                (lb.at[:, lanes_at(c, half)], row.at[0:1, 0:half]),
                (la.at[:, lanes_at(a, pb)], row.at[1:2, 0:pb]),
                (tm.at[:, lanes_at(a, pb)], row.at[2:3, 0:pb]),
            ] + [(x.at[:, lanes_at(a ^ k, pb)], blocks[k]) for k in range(A)]
            copies = [pltpu.make_async_copy(p, q, sems.at[n]) for n, (p, q) in enumerate(pairs)]
            for copy in copies:
                copy.start()
            for copy in copies:
                copy.wait()
            kept[fs : fs + 8, :] = jnp.broadcast_to(row[0:1, 0:half], (8, half))
            side[0:4, :] = jnp.broadcast_to(row[1:2, 0:pb], (4, pb))
            side[4:8, :] = jnp.broadcast_to(row[2:3, 0:pb], (4, pb))

        outs = (sds(fs, half), sds(fs + 8, half), *(sds(ft, pb) for _ in range(A)), sds(8, pb))
        out = pl.pallas_call(
            body,
            in_specs=[pl.BlockSpec(memory_space=pltpu.MemorySpace.HBM)] * 5,
            out_shape=outs,
            scratch_shapes=(pltpu.VMEM((8, max(half, pb)), F32), pltpu.SemaphoreType.DMA((5 + A,))),
            compiler_params=pltpu.CompilerParams(vmem_limit_bytes=8 * MB),
        )(*(
            pltpu.with_memory_space_constraint(v, pltpu.MemorySpace.HBM)
            for v in (sources, targets, source_logw[None], target_logw[None], times[None])
        ))
        return out[0], out[1], out[2 : 2 + A], out[2 + A]

    def cross(self, own, other, pieces):
        F, M, N, A, Y, fs, ft, half, pb, nl = (
            self.F, self.M, self.N, self.A, self.Y, self.fs, self.ft, self.half, self.pb, self.nl,
        )

        def body(own, other, *refs):
            few = len(pieces)
            s_ref, xt_ref, yh_ref, yl_ref, hy_ref, rowc_ref, logb_ref, stat_ref = refs[few : few + 8]
            x_ref, y_ref, xh_ref, xl_ref = refs[few + 8 :]
            y, c, a, b = position()
            for k in range(A):
                for q in range(2):
                    at = rows_at((a ^ k) * 2 + (b ^ q), ft)
                    src = slice((q * A + k) * ft, (q * A + k + 1) * ft)
                    x_ref[at, lanes_at(c, pb)] = own[src, :]
                    x_ref[at, lanes_at(1 - c, pb)] = other[src, :]
            for row in range(2):
                rowc_ref[row : row + 1, lanes_at(c, pb)] = own[F + 4 * row : F + 4 * row + 1, :]
                rowc_ref[row : row + 1, lanes_at(1 - c, pb)] = other[F + 4 * row : F + 4 * row + 1, :]
            for (k, m, near, away, _), p in zip(pieces, refs):
                cols = lanes_at(a ^ k, half)
                if near:
                    y_ref[rows_at((y ^ m) * 2 + c, fs), cols] = p[0:fs, :]
                    if m == 0:
                        logb_ref[0:1, cols] = p[fs : fs + 1, :]
                if away:
                    at = fs + 8 if near else 0
                    y_ref[rows_at((y ^ m) * 2 + (1 - c), fs), cols] = p[at : at + fs, :]
            for j in range(N // 256):
                cols = slice(j * 256, (j + 1) * 256)
                v = y_ref[:, cols]
                hy_ref[0:1, cols] = (0.5 * L) * jnp.sum(v * v, 0, keepdims=True)
                yh_ref[:, cols], yl_ref[:, cols] = split(v)
            for r in range(self.nr):
                rows = slice(r * LANES, (r + 1) * LANES)
                v = x_ref[:, rows]
                rowc_ref[2:3, rows] = (0.5 * L) * jnp.sum(v * v, 0, keepdims=True)
                vt = v.T
                xt_ref[rows, :] = vt
                xh_ref[rows, :], xl_ref[rows, :] = split(vt * L)
            wide = 512
            deep = min(256, M)
            for r in range(M // deep):
                rows = slice(r * deep, (r + 1) * deep)
                for j in range(N // wide):
                    cols = slice(j * wide, (j + 1) * wide)
                    s = dot3(xh_ref[rows, :], xl_ref[rows, :], yh_ref[:, cols], yl_ref[:, cols], ((1,), (0,)))
                    s_ref[rows, cols] = s - hy_ref[0:1, cols]
                for h in range(deep // LANES):
                    at = r * deep + h * LANES
                    sub = slice(at, at + LANES)
                    top = s_ref[sub, 0:LANES]
                    for l in range(1, nl):
                        top = jnp.maximum(top, s_ref[sub, l * LANES : (l + 1) * LANES])
                    peak = jnp.broadcast_to(jnp.max(top, 1, keepdims=True), (LANES, LANES))
                    acc = jnp.zeros((LANES, LANES), F32)
                    for l in range(nl):
                        acc = acc + jnp.exp2(s_ref[sub, l * LANES : (l + 1) * LANES] - peak)
                    stat_ref[0:1, sub] = jnp.max(top.T, 0, keepdims=True)
                    stat_ref[1:2, sub] = jnp.sum(acc.T, 0, keepdims=True)

        outs = (
            sds(M, N), sds(M, F), sds(F, N, dtype=BF16), sds(F, N, dtype=BF16), sds(1, N), sds(3, M), sds(1, N), sds(2, M),
        )
        scratch = (pltpu.VMEM((F, M), F32), pltpu.VMEM((F, N), F32), pltpu.VMEM((M, F), BF16), pltpu.VMEM((M, F), BF16))
        return call(body, outs, scratch, 20)(own, other, *(p[-1] for p in pieces))

    def fill_cols(self, col_ref, row):
        for r in range(self.nr):
            sub = slice(r * LANES, (r + 1) * LANES)
            col_ref[sub, :] = to_col(row[:, sub])

    def online(self, v, l, m_ref, e_ref):
        lane = slice(l * LANES, (l + 1) * LANES)
        g = groups(v)
        old = m_ref[:, lane]
        new = jnp.maximum(old, jnp.max(g, 0))
        e_ref[:, lane] = e_ref[:, lane] * jnp.exp2(old - new) + jnp.sum(jnp.exp2(g - new[None]), 0)
        m_ref[:, lane] = new

    def finish(self, m_ref, e_ref, out_ref):
        m = m_ref[...]
        top = jnp.max(m, 0, keepdims=True)
        out_ref[0:1, :] = top
        out_ref[1:2, :] = jnp.sum(e_ref[...] * jnp.exp2(m - top), 0, keepdims=True)

    def start(self, m_ref, e_ref):
        m_ref[...] = jnp.full((8, self.N), -1e30, F32)
        e_ref[...] = jnp.zeros((8, self.N), F32)

    def stats(self):
        return pltpu.VMEM((8, self.N), F32), pltpu.VMEM((8, self.N), F32)

    def cols(self):
        return pltpu.VMEM((self.M, LANES), F32)

    def col1(self, s, rowc, stats):
        def body(s_ref, rowc, *refs):
            stats, (f_ref, out_ref, col_ref, m_ref, e_ref) = refs[:-5], refs[-5:]
            f = rowc[0:1, :] * LOG2E - lse2(stats)
            f_ref[...] = f
            self.fill_cols(col_ref, f)
            self.start(m_ref, e_ref)

            @pl.loop(0, self.nr)
            def _(r):
                rows = pl.ds(pl.multiple_of(r * LANES, LANES), LANES)
                fc = col_ref[rows, :]
                for l in range(self.nl):
                    self.online(s_ref[rows, l * LANES : (l + 1) * LANES] + fc, l, m_ref, e_ref)

            self.finish(m_ref, e_ref, out_ref)

        return call(body, (sds(1, self.M), sds(2, self.N)), (self.cols(), *self.stats()), 10)(s, rowc, *stats)

    def row2(self, s, f, logb, stats):
        def body(s_ref, f, logb, *refs):
            stats, (g_ref, out_ref, col_ref) = refs[:-3], refs[-3:]
            g_ref[...] = logb[...] * LOG2E - lse2(stats)
            self.fill_cols(col_ref, f)
            for r in range(self.nr):
                rows = slice(r * LANES, (r + 1) * LANES)
                fc = col_ref[rows, :]
                acc = jnp.zeros((LANES, LANES), F32)
                for l in range(self.nl):
                    lane = slice(l * LANES, (l + 1) * LANES)
                    acc = acc + jnp.exp2(s_ref[rows, lane] + fc + g_ref[:, lane])
                out_ref[0:1, rows] = jnp.sum(acc.T, 0, keepdims=True)

        return call(body, (sds(1, self.N), sds(1, self.M)), (self.cols(),), 10)(s, f, logb, *stats)

    def col2(self, s, f, g, rowc, sums):
        def body(s_ref, f, g, rowc, *refs):
            sums, (f_ref, out_ref, col_ref, acc_ref) = refs[:-4], refs[-4:]
            f2 = f[...] + rowc[0:1, :] * LOG2E - log2(total(sums))
            f_ref[...] = f2
            self.fill_cols(col_ref, f2)
            acc_ref[...] = jnp.zeros((8, self.N), F32)

            @pl.loop(0, self.nr)
            def _(r):
                rows = pl.ds(pl.multiple_of(r * LANES, LANES), LANES)
                fc = col_ref[rows, :]
                for l in range(self.nl):
                    lane = slice(l * LANES, (l + 1) * LANES)
                    p = jnp.exp2(s_ref[rows, lane] + fc + g[:, lane])
                    acc_ref[:, lane] = acc_ref[:, lane] + jnp.sum(groups(p), 0)

            out_ref[...] = jnp.sum(acc_ref[...], 0, keepdims=True)

        scratch = (self.cols(), self.stats()[0])
        return call(body, (sds(1, self.M), sds(1, self.N)), scratch, 10)(s, f, g, rowc, *sums)

    def plan(self, s, f, g, sums, logb, yh, yl, mine, q, base):
        N, F, qr, mw = self.N, self.F, self.qr, self.mw

        def body(s_ref, f, g, logb, yh, yl, *rest):
            few = len(sums)
            parts, extra, (w_ref, g_ref, ph_ref, pl_ref) = rest[:few], rest[few:-4], rest[-4:]
            _, c, _, _ = position()
            at = (c if mine else 1 - c) * self.pb + q * qr
            g_ref[...] = g[...] + logb[...] * LOG2E - log2(total(parts))
            for r in range(qr // LANES):
                fc = to_col(f[0:1, pl.ds(pl.multiple_of(at + r * LANES, LANES), LANES)])
                rows = pl.ds(pl.multiple_of(at + r * LANES, LANES), LANES)
                local = slice(r * LANES, (r + 1) * LANES)
                acc = jnp.zeros((LANES, LANES), F32)
                for l in range(self.nl):
                    lane = slice(l * LANES, (l + 1) * LANES)
                    p = jnp.exp2(s_ref[rows, lane] + fc + g_ref[:, lane])
                    acc = acc + p
                    ph_ref[local, lane], pl_ref[local, lane] = split(p)
                i, j = divmod(r * LANES, mw)
                mass = jnp.sum(acc.T, 0, keepdims=True)
                if extra:
                    mass = mass + extra[0][qr + i : qr + i + 1, j : j + LANES]
                w_ref[qr + i : qr + i + 1, j : j + LANES] = mass
            w = dot3(ph_ref[...], pl_ref[...], yh[...], yl[...], ((1,), (1,)))
            w_ref[0:qr, :] = w + extra[0][0:qr, :] if extra else w

        scratch = (pltpu.VMEM((1, N), F32), pltpu.VMEM((qr, N), BF16), pltpu.VMEM((qr, N), BF16))
        args = (s, f, g, logb, yh, yl, *sums) + (() if base is None else (base,))
        return call(body, sds(qr + 8, F), scratch, 14)(*args)

    def last(self, own, other, xt, f, rowc, yh, yl, hy, q):
        F, M, N, A, ft, pb, qr, mw = self.F, self.M, self.N, self.A, self.ft, self.pb, self.qr, self.mw

        def entry(*refs):
            ins, outs, (m_ref, e_ref, mt_ref) = refs[:8], refs[8:-3], refs[-3:]
            parcels, out_ref = outs[:A], outs[A]
            body(*ins, parcels, out_ref, m_ref, e_ref, mt_ref)

        def body(own, other, xt, f, rowc, yh, yl, hy, parcels, out_ref, m_ref, e_ref, mt_ref):
            _, c, a, b = position()
            self.start(m_ref, e_ref)
            wide = min(512, N)
            for src, core in ((own, c), (other, 1 - c)):
                for r in range(qr // LANES):
                    at = pl.ds(pl.multiple_of(core * pb + (q * qr + r * LANES), LANES), LANES)
                    i, j = divmod(r * LANES, mw)
                    t = rowc[1:2, at]
                    nx = rowc[2:3, at]
                    keep = jnp.tile(to_col(1.0 - t), (1, F // LANES))
                    take = jnp.tile(to_col(t / src[qr + i : qr + i + 1, j : j + LANES]), (1, F // LANES))
                    mv = keep * xt[at, :] + take * src[r * LANES : (r + 1) * LANES, :]
                    mt = mv.T
                    if src is own:
                        lane = slice(r * LANES, (r + 1) * LANES)
                        mt_ref[:, lane] = mt
                        for k in range(A):
                            parcels[k][ft : ft + 8, lane] = jnp.broadcast_to((EPS * LN2) * (f[0:1, at] + nx), (8, LANES))
                    fc = to_col(f[0:1, at] + nx - (0.5 * L) * jnp.sum(mt * mt, 0, keepdims=True))
                    mh, ml = split(mv * L)
                    for n in range(N // wide):
                        cols = slice(n * wide, (n + 1) * wide)
                        v = dot3(mh, ml, yh[:, cols], yl[:, cols], ((1,), (0,))) - hy[0:1, cols]
                        for l in range(wide // LANES):
                            lane = slice(l * LANES, (l + 1) * LANES)
                            self.online(v[:, lane] + fc, n * (wide // LANES) + l, m_ref, e_ref)
            for k in range(A):
                parcels[k][0:ft, :] = mt_ref[rows_at((a ^ k) * 2 + b, ft), :]
            self.finish(m_ref, e_ref, out_ref)

        outs = (*(sds(ft + 8, qr) for _ in range(A)), sds(2, N))
        out = call(entry, outs, (*self.stats(), pltpu.VMEM((F, qr), F32)), 14)(own, other, xt, f, rowc, yh, yl, hy)
        return out[:A], out[A]

    def pack(self, parcels, stats):
        A, ft, qr, half, hw, tail = self.A, self.ft, self.qr, self.half, self.hw, self.tail

        def body(*refs):
            parts, stats, outs, st = refs[:A], refs[A : -1 - A], refs[-1 - A : -1], refs[-1]
            _, _, a, _ = position()
            st[0:1, :], st[1:2, :] = joined(stats)
            for k in range(A):
                outs[k][0 : ft + 8, :] = parts[k][...]
                for i in range(half // hw):
                    at = pl.ds(pl.multiple_of((a ^ k) * half + i * hw, LANES), hw)
                    outs[k][ft + 1 + 2 * i : ft + 3 + 2 * i, 0:hw] = st[0:2, at]

        outs = tuple(sds(ft + tail, qr) for _ in range(A))
        return call(body, outs, (pltpu.VMEM((2, self.N), F32),), 8)(*parcels, *stats)

    def unpack(self, got, kept):
        A, Q, fs, ft, pb, qr, half, hw = self.A, self.Q, self.fs, self.ft, self.pb, self.qr, self.half, self.hw

        def body(*refs):
            got, kept, moved, row_pot, pot = refs[: A * Q], refs[A * Q], refs[-3], refs[-2], refs[-1]
            _, _, a, _ = position()
            for q in range(Q):
                for k in range(A):
                    cols = pl.ds(pl.multiple_of((a ^ k) * pb + q * qr, LANES), qr)
                    moved[:, cols] = got[q * A + k][0:ft, :]
                    row_pot[0:1, cols] = got[q * A + k][ft : ft + 1, :]
            for i in range(half // hw):
                at = slice(ft + 1 + 2 * i, ft + 3 + 2 * i)
                v = lse2([got[(Q - 1) * A + k][at, 0:hw] for k in range(A)])
                lanes = slice(i * hw, (i + 1) * hw)
                pot[0:1, lanes] = EPS * (kept[fs : fs + 1, lanes] - LN2 * v)

        return call(body, (sds(ft, A * pb), sds(1, A * pb), sds(1, half)), (), 8)(*got, kept)

    def stack(self, parts):
        def body(*refs):
            for k, ref in enumerate(refs[:-1]):
                refs[-1][k * self.ft : (k + 1) * self.ft, :] = ref[...]

        return call(body, sds(len(parts) * self.ft, self.pb), (), 8)(*parts)

    def both(self, w, far):
        def body(p, q, out):
            out[...] = p[...] + q[...]

        return call(body, sds(self.qr + 8, self.F), (), 8)(w, far)

    def pair(self, pot, far):
        def body(p, q, out):
            _, c, _, _ = position()
            out[0:1, lanes_at(c, self.half)] = p[...]
            out[0:1, lanes_at(1 - c, self.half)] = q[...]

        return call(body, sds(1, 2 * self.half), (), 8)(pot, far)


def solution(mesh):
    S, T = mesh.shape["src"], mesh.shape["tgt"]
    Y, A = S // 2, T // 2

    def swap(v, axis, size, k):
        return lax.ppermute(v, axis, [(i, i ^ k) for i in range(size)])

    def over_c(v):
        return swap(v, "src", S, 1)

    def over_y(v, k):
        return swap(v, "src", S, 2 * k)

    def over_b(v):
        return swap(v, "tgt", T, 1)

    def over_a(v, k):
        return swap(v, "tgt", T, 2 * k)

    def join(p, q):
        return jnp.concatenate(joined([p, q]))

    def add(p, q):
        return p + q

    def bits(size):
        return [1 << i for i in range(size.bit_length() - 1)]

    def along_y(v, op):
        for k in bits(Y)[:-1]:
            v = op(v, over_y(v, k))
        return [v, over_y(v, bits(Y)[-1])] if Y > 1 else [v]

    def over_rows(v, op):
        v = op(v, over_c(v))
        return [v, over_b(v)]

    def over_cols(v, op):
        v = along_y(v, op)
        v = op(*v) if Y > 1 else v[0]
        return [v] + [over_a(v, k) for k in range(A - 1, 0, -1)]

    def per_device(sources, targets, source_logw, target_logw, times):
        ft, ns = sources.shape
        fs, nt = targets.shape
        half, pb = nt // 2, ns // A
        Q = 2 if pb % 256 == 0 else 1
        kern = Kernels(ft * T, fs, ft, A, Y, half, pb, Q)

        sent, kept, blocks, side = kern.prep(sources, targets, source_logw, target_logw, times)
        away = over_c(sent)
        whole = [(True, True, jnp.concatenate([kept, away]))]
        halves = [(True, False, kept), (False, True, away)]

        chunks = {0: whole}
        for bit in reversed(bits(A)):
            for k in list(chunks):
                chunks[k ^ bit] = []
                for near, far, v in halves if k == 0 and bit == A // 2 else chunks[k]:
                    chunks[k ^ bit].append((near, far, over_a(v, bit)))
        pieces = []
        for k in range(A):
            for near, far, v in chunks[k]:
                pieces.append((k, 0, near, far, v))
                for m in range(1, Y):
                    pieces.append((k, m, near, far, over_y(v, m)))
        parts = [blocks[0]]
        for k in range(1, A):
            parts.append(over_a(blocks[k], k))
        xs = kern.stack(parts)
        xb = over_b(xs)
        x_own = jnp.concatenate([xs, xb, side])
        x_other = over_c(x_own)

        sc, xt, yh, yl, hy, rowc, logb, stat = kern.cross(x_own, x_other, pieces)
        f1, stat = kern.col1(sc, rowc, over_rows(stat, join))
        g1, sums = kern.row2(sc, f1, logb, over_cols(stat, join))
        f2, sums = kern.col2(sc, f1, g1, rowc, over_rows(sums, add))
        sums = over_cols(sums, add)

        def plan(mine, q, base):
            return kern.plan(sc, f2, g1, sums, logb, yh, yl, mine, q, base)

        theirs = [over_c(plan(False, q, None)) for q in range(Q)]
        got, stat = [], None
        for q in range(Q):
            w = plan(True, q, theirs[q])
            far = over_b(w)
            w = kern.both(w, far)
            far = over_c(w)
            parcels, fresh = kern.last(w, far, xt, f2, rowc, yh, yl, hy, q)
            stat = fresh if stat is None else join(stat, fresh)
            if q == Q - 1:
                parcels = kern.pack(parcels, along_y(stat, join))
            got.append(parcels[0])
            for k in range(1, A):
                got.append(over_a(parcels[k], k))
        moved, row_pot, pot = kern.unpack(got, kept)
        col_pot = kern.pair(pot, over_c(pot))
        return row_pot[0], moved, col_pot[0]

    placed = (P("tgt", "src"), P("src", "tgt"), P("src"), P("tgt"), P("src"))
    return jax.shard_map(
        per_device,
        mesh=mesh,
        in_specs=placed,
        out_specs=(P("src"), P("tgt", "src"), P("tgt")),
        check_vma=False,
    )
```

```python
import jax
import jax.numpy as jnp
from jax import lax
from jax.experimental import pallas as pl
from jax.experimental.pallas import tpu as pltpu
from jax.sharding import PartitionSpec as P


EPS = 16.0
LOG2E = 1.4426950408889634
LN2 = 0.6931471805599453
L = LOG2E / EPS
LANES = 128
F32 = jnp.float32
BF16 = jnp.bfloat16
MB = 1024 * 1024


def split(v):
    hi = v.astype(BF16)
    return hi, (v - hi.astype(F32)).astype(BF16)


def dot3(ah, al, bh, bl, dims):
    d = lambda p, q: lax.dot_general(p, q, (dims, ((), ())), preferred_element_type=F32)
    return d(ah, bh) + d(ah, bl) + d(al, bh)


def to_col(row):
    return jnp.broadcast_to(row, (LANES, LANES)).T


def log2(v):
    return jnp.log(v) * LOG2E


def groups(v):
    return v.reshape(v.shape[0] // 8, 8, v.shape[1])


def call(body, outs, scratch, limit):
    return pl.pallas_call(
        body,
        out_shape=outs,
        scratch_shapes=scratch,
        compiler_params=pltpu.CompilerParams(vmem_limit_bytes=limit * MB),
    )


def sds(*shape, dtype=F32):
    return jax.ShapeDtypeStruct(shape, dtype)


def position():
    s, t = lax.axis_index("src"), lax.axis_index("tgt")
    return s >> 1, s & 1, t >> 1, t & 1


def lanes_at(index, size):
    return pl.ds(pl.multiple_of(index * size, LANES), size)


def rows_at(index, size):
    return pl.ds(pl.multiple_of(index * size, 8), size)


def joined(values):
    top = values[0][0:1, :]
    for v in values[1:]:
        top = jnp.maximum(top, v[0:1, :])
    return top, total([v[1:2, :] * jnp.exp2(v[0:1, :] - top) for v in values])


def total(values):
    acc = values[0][...]
    for v in values[1:]:
        acc = acc + v[...]
    return acc


def lse2(values):
    top, acc = joined(values)
    return top + log2(acc)


class Kernels:
    def __init__(self, F, fs, ft, A, Y, half, pb, Q):
        self.F, self.fs, self.ft, self.A, self.Y, self.half, self.pb, self.Q = F, fs, ft, A, Y, half, pb, Q
        self.M, self.N = 2 * pb, A * half
        self.nl, self.nr = self.N // LANES, self.M // LANES
        self.qr = pb // Q
        self.mw = min(self.qr, F)
        self.hw = min(half, self.qr)
        self.tail = -(-(1 + 2 * (half // self.hw)) // 8) * 8

    def prep(self, sources, targets, source_logw, target_logw, times):
        fs, ft, A, half, pb = self.fs, self.ft, self.A, self.half, self.pb

        def body(x, v, la, lb, tm, sent, kept, *rest):
            blocks, side, row, sems = rest[:A], rest[A], rest[A + 1], rest[A + 2]
            _, c, a, _ = position()
            pairs = [
                (v.at[:, lanes_at(1 - c, half)], sent),
                (v.at[:, lanes_at(c, half)], kept.at[0:fs, :]),
                (lb.at[:, lanes_at(c, half)], row.at[0:1, 0:half]),
                (la.at[:, lanes_at(a, pb)], row.at[1:2, 0:pb]),
                (tm.at[:, lanes_at(a, pb)], row.at[2:3, 0:pb]),
            ] + [(x.at[:, lanes_at(a ^ k, pb)], blocks[k]) for k in range(A)]
            copies = [pltpu.make_async_copy(p, q, sems.at[n]) for n, (p, q) in enumerate(pairs)]
            for copy in copies:
                copy.start()
            for copy in copies:
                copy.wait()
            kept[fs : fs + 8, :] = jnp.broadcast_to(row[0:1, 0:half], (8, half))
            side[0:4, :] = jnp.broadcast_to(row[1:2, 0:pb], (4, pb))
            side[4:8, :] = jnp.broadcast_to(row[2:3, 0:pb], (4, pb))

        outs = (sds(fs, half), sds(fs + 8, half), *(sds(ft, pb) for _ in range(A)), sds(8, pb))
        out = pl.pallas_call(
            body,
            in_specs=[pl.BlockSpec(memory_space=pltpu.MemorySpace.HBM)] * 5,
            out_shape=outs,
            scratch_shapes=(pltpu.VMEM((8, max(half, pb)), F32), pltpu.SemaphoreType.DMA((5 + A,))),
            compiler_params=pltpu.CompilerParams(vmem_limit_bytes=8 * MB),
        )(*(
            pltpu.with_memory_space_constraint(v, pltpu.MemorySpace.HBM)
            for v in (sources, targets, source_logw[None], target_logw[None], times[None])
        ))
        return out[0], out[1], out[2 : 2 + A], out[2 + A]

    def rows(self, own, other):
        F, M, A, ft, pb = self.F, self.M, self.A, self.ft, self.pb

        def body(own, other, xt_ref, xh_ref, xl_ref, rowc_ref, x_ref):
            _, c, a, b = position()
            for k in range(A):
                for q in range(2):
                    at = rows_at((a ^ k) * 2 + (b ^ q), ft)
                    src = slice((q * A + k) * ft, (q * A + k + 1) * ft)
                    x_ref[at, lanes_at(c, pb)] = own[src, :]
                    x_ref[at, lanes_at(1 - c, pb)] = other[src, :]
            for row in range(2):
                rowc_ref[row : row + 1, lanes_at(c, pb)] = own[F + 4 * row : F + 4 * row + 1, :]
                rowc_ref[row : row + 1, lanes_at(1 - c, pb)] = other[F + 4 * row : F + 4 * row + 1, :]
            for r in range(self.nr):
                rows = slice(r * LANES, (r + 1) * LANES)
                v = x_ref[:, rows]
                rowc_ref[2:3, rows] = (0.5 * L) * jnp.sum(v * v, 0, keepdims=True)
                vt = v.T
                xt_ref[rows, :] = vt
                xh_ref[rows, :], xl_ref[rows, :] = split(vt * L)

        outs = (sds(M, F), sds(M, F, dtype=BF16), sds(M, F, dtype=BF16), sds(3, M))
        return call(body, outs, (pltpu.VMEM((F, M), F32),), 10)(own, other)

    def cross(self, xh, xl, pieces, before):
        F, M, fs, half = self.F, self.M, self.fs, self.half
        nb = half // LANES

        def body(xh_ref, xl_ref, *refs):
            few = len(pieces)
            parts, prior = refs[:few], refs[few : few + len(before)]
            s_ref, yh_ref, yl_ref, hy_ref, logb_ref, stat_ref, y_ref = refs[few + len(before) :]
            y, c, _, _ = position()
            for (m, near, away, _), p in zip(pieces, parts):
                if near:
                    y_ref[rows_at((y ^ m) * 2 + c, fs), :] = p[0:fs, :]
                    if m == 0:
                        logb_ref[...] = p[fs : fs + 1, :] * LOG2E
                if away:
                    at = fs + 8 if near else 0
                    y_ref[rows_at((y ^ m) * 2 + (1 - c), fs), :] = p[at : at + fs, :]
            for j in range(half // LANES):
                cols = slice(j * LANES, (j + 1) * LANES)
                v = y_ref[:, cols]
                hy_ref[0:1, cols] = (0.5 * L) * jnp.sum(v * v, 0, keepdims=True)
                yh_ref[:, cols], yl_ref[:, cols] = split(v)
            deep = min(256, M)
            for r in range(M // deep):
                rows = slice(r * deep, (r + 1) * deep)
                s = dot3(xh_ref[rows, :], xl_ref[rows, :], yh_ref[...], yl_ref[...], ((1,), (0,)))
                s_ref[rows, :] = s - hy_ref[...]
                for h in range(deep // LANES):
                    at = r * deep + h * LANES
                    sub = slice(at, at + LANES)
                    top = s_ref[sub, 0:LANES]
                    for l in range(1, nb):
                        top = jnp.maximum(top, s_ref[sub, l * LANES : (l + 1) * LANES])
                    peak = jnp.broadcast_to(jnp.max(top, 1, keepdims=True), (LANES, LANES))
                    acc = jnp.zeros((LANES, LANES), F32)
                    for l in range(nb):
                        acc = acc + jnp.exp2(s_ref[sub, l * LANES : (l + 1) * LANES] - peak)
                    stat_ref[0:1, sub] = jnp.max(top.T, 0, keepdims=True)
                    stat_ref[1:2, sub] = jnp.sum(acc.T, 0, keepdims=True)
            if before:
                top, acc = joined([stat_ref[...]] + [v[...] for v in prior])
                stat_ref[0:1, :] = top
                stat_ref[1:2, :] = acc

        outs = (
            sds(M, half), sds(F, half, dtype=BF16), sds(F, half, dtype=BF16), sds(1, half), sds(1, half), sds(2, M),
        )
        return call(body, outs, (pltpu.VMEM((F, half), F32),), 10)(xh, xl, *(p[-1] for p in pieces), *before)

    def blocks(self):
        nb = self.half // LANES
        return [(k, slice(l * LANES, (l + 1) * LANES), k * nb + l) for k in range(self.A) for l in range(nb)]

    def chunk(self, k):
        _, _, a, _ = position()
        return lanes_at(a ^ k, self.half)

    def own_order(self, k):
        return slice(k * self.half, (k + 1) * self.half)

    def fill_cols(self, col_ref, row):
        for r in range(self.nr):
            sub = slice(r * LANES, (r + 1) * LANES)
            col_ref[sub, :] = to_col(row[:, sub])

    def online(self, v, l, m_ref, e_ref):
        lane = slice(l * LANES, (l + 1) * LANES)
        g = groups(v)
        old = m_ref[:, lane]
        new = jnp.maximum(old, jnp.max(g, 0))
        e_ref[:, lane] = e_ref[:, lane] * jnp.exp2(old - new) + jnp.sum(jnp.exp2(g - new[None]), 0)
        m_ref[:, lane] = new

    def finish(self, m_ref, e_ref, out_ref):
        for k in range(self.A):
            m = m_ref[:, self.own_order(k)]
            top = jnp.max(m, 0, keepdims=True)
            out_ref[0:1, self.chunk(k)] = top
            out_ref[1:2, self.chunk(k)] = jnp.sum(e_ref[:, self.own_order(k)] * jnp.exp2(m - top), 0, keepdims=True)

    def start(self, m_ref, e_ref):
        m_ref[...] = jnp.full((8, self.N), -1e30, F32)
        e_ref[...] = jnp.zeros((8, self.N), F32)

    def stats(self):
        return pltpu.VMEM((8, self.N), F32), pltpu.VMEM((8, self.N), F32)

    def cols(self):
        return pltpu.VMEM((self.M, LANES), F32)

    def col1(self, s, rowc, stats):
        A = self.A

        def body(*refs):
            s_refs, rowc, stats, (f_ref, out_ref, col_ref, m_ref, e_ref) = refs[:A], refs[A], refs[A + 1 : -5], refs[-5:]
            f = rowc[0:1, :] * LOG2E - lse2(stats)
            f_ref[...] = f
            self.fill_cols(col_ref, f)
            self.start(m_ref, e_ref)

            @pl.loop(0, self.nr)
            def _(r):
                rows = pl.ds(pl.multiple_of(r * LANES, LANES), LANES)
                fc = col_ref[rows, :]
                for k, lane, l in self.blocks():
                    self.online(s_refs[k][rows, lane] + fc, l, m_ref, e_ref)

            self.finish(m_ref, e_ref, out_ref)

        return call(body, (sds(1, self.M), sds(2, self.N)), (self.cols(), *self.stats()), 10)(*s, rowc, *stats)

    def row2(self, s, f, logb, stats):
        A = self.A

        def body(*refs):
            s_refs, f, logb, stats, (g_ref, out_ref, col_ref) = refs[:A], refs[A], refs[A + 1 : 2 * A + 1], refs[2 * A + 1 : -3], refs[-3:]
            for k in range(A):
                g_ref[:, self.own_order(k)] = logb[k][...] - lse2([v[:, self.chunk(k)] for v in stats])
            self.fill_cols(col_ref, f)
            for r in range(self.nr):
                rows = slice(r * LANES, (r + 1) * LANES)
                fc = col_ref[rows, :]
                acc = jnp.zeros((LANES, LANES), F32)
                for k, lane, l in self.blocks():
                    acc = acc + jnp.exp2(s_refs[k][rows, lane] + fc + g_ref[:, l * LANES : (l + 1) * LANES])
                out_ref[0:1, rows] = jnp.sum(acc.T, 0, keepdims=True)

        return call(body, (sds(1, self.N), sds(1, self.M)), (self.cols(),), 10)(*s, f, *logb, *stats)

    def col2(self, s, f, g, rowc, sums):
        A = self.A

        def body(*refs):
            s_refs, f, g, rowc = refs[:A], refs[A], refs[A + 1], refs[A + 2]
            sums, (f_ref, out_ref, col_ref, acc_ref) = refs[A + 3 : -4], refs[-4:]
            f2 = f[...] + rowc[0:1, :] * LOG2E - log2(total(sums))
            f_ref[...] = f2
            self.fill_cols(col_ref, f2)
            acc_ref[...] = jnp.zeros((8, self.N), F32)

            @pl.loop(0, self.nr)
            def _(r):
                rows = pl.ds(pl.multiple_of(r * LANES, LANES), LANES)
                fc = col_ref[rows, :]
                for k, lane, l in self.blocks():
                    at = slice(l * LANES, (l + 1) * LANES)
                    p = jnp.exp2(s_refs[k][rows, lane] + fc + g[:, at])
                    acc_ref[:, at] = acc_ref[:, at] + jnp.sum(groups(p), 0)

            for k in range(A):
                out_ref[0:1, self.chunk(k)] = jnp.sum(acc_ref[:, self.own_order(k)], 0, keepdims=True)

        scratch = (self.cols(), self.stats()[0])
        return call(body, (sds(1, self.M), sds(1, self.N)), scratch, 10)(*s, f, g, rowc, *sums)

    def plan(self, s, f, g, sums, logb, yh, yl, mine, q, base):
        N, F, A, qr, mw = self.N, self.F, self.A, self.qr, self.mw

        def body(*refs):
            s_refs, logb, yh, yl, (f, g), rest = (
                refs[:A], refs[A : 2 * A], refs[2 * A : 3 * A], refs[3 * A : 4 * A], refs[4 * A : 4 * A + 2], refs[4 * A + 2 :],
            )
            few = len(sums)
            parts, extra, (w_ref, g_ref, ph_ref, pl_ref) = rest[:few], rest[few:-4], rest[-4:]
            _, c, _, _ = position()
            at = (c if mine else 1 - c) * self.pb + q * qr
            for k in range(A):
                cols = self.own_order(k)
                g_ref[:, cols] = g[:, cols] + logb[k][...] - log2(total([v[:, self.chunk(k)] for v in parts]))
            for r in range(qr // LANES):
                rows = pl.ds(pl.multiple_of(at + r * LANES, LANES), LANES)
                fc = to_col(f[0:1, rows])
                local = slice(r * LANES, (r + 1) * LANES)
                acc = jnp.zeros((LANES, LANES), F32)
                for k, lane, l in self.blocks():
                    cols = slice(l * LANES, (l + 1) * LANES)
                    p = jnp.exp2(s_refs[k][rows, lane] + fc + g_ref[:, cols])
                    acc = acc + p
                    ph_ref[local, cols], pl_ref[local, cols] = split(p)
                i, j = divmod(r * LANES, mw)
                mass = jnp.sum(acc.T, 0, keepdims=True)
                if extra:
                    mass = mass + extra[0][qr + i : qr + i + 1, j : j + LANES]
                w_ref[qr + i : qr + i + 1, j : j + LANES] = mass
            w = None
            for k in range(A):
                cols = self.own_order(k)
                d = dot3(ph_ref[:, cols], pl_ref[:, cols], yh[k][...], yl[k][...], ((1,), (1,)))
                w = d if w is None else w + d
            w_ref[0:qr, :] = w + extra[0][0:qr, :] if extra else w

        scratch = (pltpu.VMEM((1, N), F32), pltpu.VMEM((qr, N), BF16), pltpu.VMEM((qr, N), BF16))
        args = (*s, *logb, *yh, *yl, f, g, *sums) + (() if base is None else (base,))
        return call(body, sds(qr + 8, F), scratch, 14)(*args)

    def last(self, own, other, xt, f, rowc, yh, yl, hy, q):
        F, M, N, A, ft, pb, qr, mw = self.F, self.M, self.N, self.A, self.ft, self.pb, self.qr, self.mw

        def entry(*refs):
            ins, ys, outs, (m_ref, e_ref, mt_ref) = refs[:5], refs[5 : 5 + 3 * A], refs[5 + 3 * A : -3], refs[-3:]
            parcels, out_ref = outs[:A], outs[A]
            body(*ins, ys[:A], ys[A : 2 * A], ys[2 * A :], parcels, out_ref, m_ref, e_ref, mt_ref)

        def body(own, other, xt, f, rowc, yh, yl, hy, parcels, out_ref, m_ref, e_ref, mt_ref):
            _, c, a, b = position()
            self.start(m_ref, e_ref)
            wide = self.half
            for src, core in ((own, c), (other, 1 - c)):
                for r in range(qr // LANES):
                    at = pl.ds(pl.multiple_of(core * pb + (q * qr + r * LANES), LANES), LANES)
                    i, j = divmod(r * LANES, mw)
                    t = rowc[1:2, at]
                    nx = rowc[2:3, at]
                    keep = jnp.tile(to_col(1.0 - t), (1, F // LANES))
                    take = jnp.tile(to_col(t / src[qr + i : qr + i + 1, j : j + LANES]), (1, F // LANES))
                    mv = keep * xt[at, :] + take * src[r * LANES : (r + 1) * LANES, :]
                    mt = mv.T
                    if src is own:
                        lane = slice(r * LANES, (r + 1) * LANES)
                        mt_ref[:, lane] = mt
                        for k in range(A):
                            parcels[k][ft : ft + 8, lane] = jnp.broadcast_to((EPS * LN2) * (f[0:1, at] + nx), (8, LANES))
                    fc = to_col(f[0:1, at] + nx - (0.5 * L) * jnp.sum(mt * mt, 0, keepdims=True))
                    mh, ml = split(mv * L)
                    for n in range(A):
                        v = dot3(mh, ml, yh[n][...], yl[n][...], ((1,), (0,))) - hy[n][...]
                        for l in range(wide // LANES):
                            lane = slice(l * LANES, (l + 1) * LANES)
                            self.online(v[:, lane] + fc, n * (wide // LANES) + l, m_ref, e_ref)
            for k in range(A):
                parcels[k][0:ft, :] = mt_ref[rows_at((a ^ k) * 2 + b, ft), :]
            self.finish(m_ref, e_ref, out_ref)

        outs = (*(sds(ft + 8, qr) for _ in range(A)), sds(2, N))
        out = call(entry, outs, (*self.stats(), pltpu.VMEM((F, qr), F32)), 14)(own, other, xt, f, rowc, *yh, *yl, *hy)
        return out[:A], out[A]

    def pack(self, parcels, stats):
        A, ft, qr, half, hw, tail = self.A, self.ft, self.qr, self.half, self.hw, self.tail

        def body(*refs):
            parts, stats, outs, st = refs[:A], refs[A : -1 - A], refs[-1 - A : -1], refs[-1]
            _, _, a, _ = position()
            st[0:1, :], st[1:2, :] = joined(stats)
            for k in range(A):
                outs[k][0 : ft + 8, :] = parts[k][...]
                for i in range(half // hw):
                    at = pl.ds(pl.multiple_of((a ^ k) * half + i * hw, LANES), hw)
                    outs[k][ft + 1 + 2 * i : ft + 3 + 2 * i, 0:hw] = st[0:2, at]

        outs = tuple(sds(ft + tail, qr) for _ in range(A))
        return call(body, outs, (pltpu.VMEM((2, self.N), F32),), 8)(*parcels, *stats)

    def unpack(self, got, kept):
        A, Q, fs, ft, pb, qr, half, hw = self.A, self.Q, self.fs, self.ft, self.pb, self.qr, self.half, self.hw

        def body(*refs):
            got, kept, moved, row_pot, pot = refs[: A * Q], refs[A * Q], refs[-3], refs[-2], refs[-1]
            _, _, a, _ = position()
            for q in range(Q):
                for k in range(A):
                    cols = pl.ds(pl.multiple_of((a ^ k) * pb + q * qr, LANES), qr)
                    moved[:, cols] = got[q * A + k][0:ft, :]
                    row_pot[0:1, cols] = got[q * A + k][ft : ft + 1, :]
            for i in range(half // hw):
                at = slice(ft + 1 + 2 * i, ft + 3 + 2 * i)
                v = lse2([got[(Q - 1) * A + k][at, 0:hw] for k in range(A)])
                lanes = slice(i * hw, (i + 1) * hw)
                pot[0:1, lanes] = EPS * (kept[fs : fs + 1, lanes] - LN2 * v)

        return call(body, (sds(ft, A * pb), sds(1, A * pb), sds(1, half)), (), 8)(*got, kept)

    def stack(self, parts):
        def body(*refs):
            for k, ref in enumerate(refs[:-1]):
                refs[-1][k * self.ft : (k + 1) * self.ft, :] = ref[...]

        return call(body, sds(len(parts) * self.ft, self.pb), (), 8)(*parts)

    def both(self, w, far):
        def body(p, q, out):
            out[...] = p[...] + q[...]

        return call(body, sds(self.qr + 8, self.F), (), 8)(w, far)

    def pair(self, pot, far):
        def body(p, q, out):
            _, c, _, _ = position()
            out[0:1, lanes_at(c, self.half)] = p[...]
            out[0:1, lanes_at(1 - c, self.half)] = q[...]

        return call(body, sds(1, 2 * self.half), (), 8)(pot, far)


def solution(mesh):
    S, T = mesh.shape["src"], mesh.shape["tgt"]
    Y, A = S // 2, T // 2

    def swap(v, axis, size, k):
        return lax.ppermute(v, axis, [(i, i ^ k) for i in range(size)])

    def over_c(v):
        return swap(v, "src", S, 1)

    def over_y(v, k):
        return swap(v, "src", S, 2 * k)

    def over_b(v):
        return swap(v, "tgt", T, 1)

    def over_a(v, k):
        return swap(v, "tgt", T, 2 * k)

    def join(p, q):
        return jnp.concatenate(joined([p, q]))

    def add(p, q):
        return p + q

    def bits(size):
        return [1 << i for i in range(size.bit_length() - 1)]

    def along_y(v, op):
        for k in bits(Y)[:-1]:
            v = op(v, over_y(v, k))
        return [v, over_y(v, bits(Y)[-1])] if Y > 1 else [v]

    def over_rows(v, op):
        v = op(v, over_c(v))
        return [v, over_b(v)]

    def over_cols(v, op):
        v = along_y(v, op)
        v = op(*v) if Y > 1 else v[0]
        return [v] + [over_a(v, k) for k in range(1, A)]

    def per_device(sources, targets, source_logw, target_logw, times):
        ft, ns = sources.shape
        fs, nt = targets.shape
        half, pb = nt // 2, ns // A
        Q = 2 if pb % 256 == 0 else 1
        kern = Kernels(ft * T, fs, ft, A, Y, half, pb, Q)

        sent, kept, blocks, side = kern.prep(sources, targets, source_logw, target_logw, times)
        away = over_c(sent)
        whole = [(True, True, jnp.concatenate([kept, away]))]
        halves = [(True, False, kept), (False, True, away)]

        chunks = {0: whole}
        for bit in reversed(bits(A)):
            for k in list(chunks):
                chunks[k ^ bit] = []
                for near, far, v in halves if k == 0 and bit == A // 2 else chunks[k]:
                    chunks[k ^ bit].append((near, far, over_a(v, bit)))
        pieces = [[] for _ in range(A)]
        for k in range(A):
            for near, far, v in chunks[k]:
                pieces[k].append((0, near, far, v))
                for m in range(1, Y):
                    pieces[k].append((m, near, far, over_y(v, m)))
        parts = [blocks[0]]
        for k in range(1, A):
            parts.append(over_a(blocks[k], k))
        xs = kern.stack(parts)
        xb = over_b(xs)
        x_own = jnp.concatenate([xs, xb, side])
        x_other = over_c(x_own)

        xt, xh, xl, rowc = kern.rows(x_own, x_other)
        found, stats = [], []
        for k in range(A):
            out = kern.cross(xh, xl, pieces[k], stats if k == A - 1 else [])
            found.append(out[:-1])
            stats.append(out[-1])
        sc, yh, yl, hy, logb = zip(*found)
        stat = stats[-1]
        f1, stat = kern.col1(sc, rowc, over_rows(stat, join))
        g1, sums = kern.row2(sc, f1, logb, over_cols(stat, join))
        f2, sums = kern.col2(sc, f1, g1, rowc, over_rows(sums, add))
        sums = over_cols(sums, add)

        def plan(mine, q, base):
            return kern.plan(sc, f2, g1, sums, logb, yh, yl, mine, q, base)

        theirs = [over_c(plan(False, q, None)) for q in range(Q)]
        got, stat = [], None
        for q in range(Q):
            w = plan(True, q, theirs[q])
            far = over_b(w)
            w = kern.both(w, far)
            far = over_c(w)
            parcels, fresh = kern.last(w, far, xt, f2, rowc, yh, yl, hy, q)
            stat = fresh if stat is None else join(stat, fresh)
            if q == Q - 1:
                parcels = kern.pack(parcels, along_y(stat, join))
            got.append(parcels[0])
            for k in range(1, A):
                got.append(over_a(parcels[k], k))
        moved, row_pot, pot = kern.unpack(got, kept)
        col_pot = kern.pair(pot, over_c(pot))
        return row_pot[0], moved, col_pot[0]

    placed = (P("tgt", "src"), P("src", "tgt"), P("src"), P("tgt"), P("src"))
    return jax.shard_map(
        per_device,
        mesh=mesh,
        in_specs=placed,
        out_specs=(P("src"), P("tgt", "src"), P("tgt")),
        check_vma=False,
    )
```
